32 devices in a mesh: dp: 8 (over z, x), mp: 4 (over y, core).
Axes of the slice: x: 2, y: 2, z: 4, core: 2. Of those that a mesh axis runs over, the one named last changes fastest.
Arguments:
- grads: bfloat16 [8, 4, 4096, 256], P('dp', 'mp'), may hold values from -6 to 6
- master: float32 [4, 4096, 256], P('mp', 'dp'), may hold values from -6 to 6
- m_codes: bfloat16 [4, 4096, 256], P('mp', 'dp'), may hold values from -1 to 1
- m_scale: float32 [4, 4096], P('mp', 'dp'), may hold values from 0.005 to 0.05
- v_codes: bfloat16 [4, 4096, 256], P('mp', 'dp'), may hold values from 0.049804688 to 1
- v_scale: float32 [4, 4096], P('mp', 'dp'), may hold values from 0.001 to 0.01
Outputs:
- master_out: float32 [4, 4096, 256], P('mp', 'dp')
- m_codes_out: bfloat16 [4, 4096, 256], P('mp', 'dp')
- m_scale_out: float32 [4, 4096], P('mp', 'dp')
- v_codes_out: bfloat16 [4, 4096, 256], P('mp', 'dp')
- v_scale_out: float32 [4, 4096], P('mp', 'dp')
- weights: bfloat16 [4, 4096, 256], P('mp')
The draws below stay inside these ranges and needn't reach their ends.
All inputs are finite; a program needn't handle non-finite values. Where the reference program divides by a largest or mean magnitude, that divisor is 1e-20 or more.
Results may differ from the reference program's by a relative error of at most 0.024.
Values may be sent and summed in bfloat16 or wider, within the bound.
No kernel may reach another device: no remote copies, remote signals or barrier semaphores. Data moves between devices by JAX's collectives and lax.ppermute only.
A program may use at most 128 MiB of HBM per device.

```python
import math
import jax
import jax.numpy as jnp
from jax import lax

BLOCK = 256
OWNB = 512
STEP = 8
MPB = 4096
LEVELS = 3
N_DP = 8
N_MP = 4


def raised(array, rng, source, target, shards_of, factor):
    def block_of(dim):
        return (jnp.arange(array.shape[dim]) // (array.shape[dim] // shards_of)).reshape((-1,) + (1,) * (array.ndim - 1 - dim))

    one_side = jax.random.permutation(rng, shards_of)[block_of(target)]
    other_side = (block_of(target) + shards_of // 2) % shards_of
    return jnp.where((block_of(source) == one_side) | (block_of(source) == other_side), factor * array, array)


def level_of(stream_key, dims, cuts, smallest, largest):
    factor_of = 1.0
    for position, shards_of in cuts:
        heights = jax.random.uniform(jax.random.fold_in(jax.random.fold_in(stream_key, 6), position), (shards_of,), jnp.float32, smallest / len(cuts), largest / len(cuts))
        factor_of = factor_of * jnp.repeat(jnp.exp(heights), dims[position] // shards_of).reshape((-1,) + (1,) * (len(dims) - 1 - position))
    return factor_of


def gaussian(rng, shape, scale, bound, shards=(), kind=jnp.bfloat16):
    result = jax.random.normal(rng, shape, jnp.float32) * scale
    if len(shards) > 0:
        result = level_of(rng, shape, shards, -0.22, 0.18) * result
    return jnp.clip(result, min=-bound, max=bound).astype(kind)


def gaussian_with(key, shape, width, most, shards, heavy, kind=jnp.bfloat16):
    array = width * jax.random.normal(key, shape, jnp.float32)
    if shards:
        array = array * level_of(key, shape, shards, -0.22, 0.18)
    return jnp.clip(raised(array, jax.random.fold_in(key, 3), *heavy), -most, most).astype(kind)


def setup_inputs(seed: int = 0) -> dict:
    arg_keys = jax.random.split(jax.random.key(seed), 7)
    grads = gaussian_with(arg_keys[0], (N_DP, N_MP, MPB, BLOCK), 1.0, 6.0, ((0, 8), (1, 4)), (0, 2, 8, 2.0))
    master = gaussian(arg_keys[1], (N_MP, MPB, BLOCK), 1.0, 6.0, ((0, 4), (1, 8)), jnp.float32)
    m_codes = jnp.clip(jax.random.uniform(arg_keys[2], (N_MP, MPB, BLOCK), jnp.float32, -1.0, 1.0) * level_of(arg_keys[2], (N_MP, MPB, BLOCK), ((0, 4), (1, 8)), -0.4, 0.0), -1.0, 1.0).astype(jnp.bfloat16)
    m_scale = jnp.clip(jnp.exp(math.log(0.05) - 2.3025851 * jax.random.uniform(arg_keys[3], (N_MP, MPB), jnp.float32) ** level_of(arg_keys[3], (N_MP, MPB), ((0, 4), (1, 8)), -0.2, 0.2)), 0.005, 0.05)
    v_codes = jnp.clip(0.049804688 + 0.9501953 * jax.random.uniform(arg_keys[4], (N_MP, MPB, BLOCK), jnp.float32) ** level_of(arg_keys[4], (N_MP, MPB, BLOCK), ((0, 4), (1, 8)), -0.2, 0.2), 0.049804688, 1.0).astype(jnp.bfloat16)
    v_scale = jnp.clip(jnp.exp(math.log(0.01) - 2.30258502 * jax.random.uniform(arg_keys[5], (N_MP, MPB), jnp.float32) ** level_of(arg_keys[5], (N_MP, MPB), ((0, 4), (1, 8)), -0.2, 0.2)), 0.001, 0.01)
    return dict(grads=grads, master=master, m_codes=m_codes, m_scale=m_scale, v_codes=v_codes, v_scale=v_scale)


def block_code(values):
    scale = (lax.optimization_barrier(jnp.max(jnp.abs(values), axis=-1)) + 1e-06).astype(jnp.bfloat16)
    levels = (values / scale.astype(jnp.float32)[..., None]).astype(jnp.bfloat16)
    return (levels, scale)

def expand(levels, scale):
    return levels.astype(jnp.float32) * scale.astype(jnp.float32)[..., None]

def state_code(values):
    scale = lax.optimization_barrier(jnp.max(jnp.abs(values), axis=-1)) + 1e-06
    return ((values / scale[..., None]).astype(jnp.bfloat16), scale)

def pair_tree(values):
    for level in range(LEVELS - 1):
        pairs = values.reshape((values.shape[0] // 2, 2) + values.shape[1:])
        levels, scale = block_code(pairs[:, 0] + pairs[:, 1])
        values = expand(levels, scale)
    return values[0] + values[1]

def reference(grads, master, m_codes, m_scale, v_codes, v_scale):

    def owner_mean(index):
        shard = (index // N_DP).astype(jnp.int32)
        owner = (index % N_DP).astype(jnp.int32)
        zero = jnp.zeros((), jnp.int32)
        start = (owner * OWNB).astype(jnp.int32)
        piece = lax.dynamic_slice(grads, (zero, shard, start, zero), (N_DP, 1, OWNB, BLOCK))[:, 0]
        levels, scale = block_code(piece.astype(jnp.float32))
        return pair_tree(expand(levels, scale)) / N_DP
    indices = jnp.arange(N_MP * N_DP, dtype=jnp.int32)
    grad_mean = lax.map(owner_mean, indices).reshape(N_MP, MPB, BLOCK)
    moment_one = 0.9 * m_codes.astype(jnp.float32) * m_scale[..., None] + 0.1 * grad_mean
    moment_two = 0.95 * v_codes.astype(jnp.float32) * v_scale[..., None] + 0.05 * grad_mean * grad_mean
    first_fix = 1.0 - 0.9 ** STEP
    second_fix = 1.0 - 0.95 ** STEP
    master_out = master - 0.1 * (moment_one / first_fix) / (jnp.sqrt(moment_two / second_fix) + 1e-08)
    one_code, one_scale = state_code(moment_one)
    two_code, two_scale = state_code(moment_two)
    weights = master_out.astype(jnp.bfloat16)
    return (master_out, one_code, one_scale, two_code, two_scale, weights)
```

```python
import jax
import jax.numpy as jnp
from jax import lax
from jax.sharding import PartitionSpec as P

STEP = 8
CHUNKS = 1


def swap(piece, bit):
    pairs = [(i, i ^ bit) for i in range(lax.axis_size("dp"))]
    return lax.ppermute(piece, "dp", pairs)


def low_bit(k):
    return k & -k


def adam(total, replicas, master, m_codes, m_scale, v_codes, v_scale):
    grad_mean = total / replicas
    moment_one = 0.9 * m_codes.astype(jnp.float32) * m_scale[:, None] + 0.1 * grad_mean
    moment_two = (
        0.95 * v_codes.astype(jnp.float32) * v_scale[:, None] + 0.05 * grad_mean * grad_mean
    )
    first_fix = 1.0 - 0.9**STEP
    second_fix = 1.0 - 0.95**STEP
    master_new = master - 0.1 * (moment_one / first_fix) / (
        jnp.sqrt(moment_two / second_fix) + 1e-08
    )
    one_scale = jnp.max(jnp.abs(moment_one), axis=-1) + 1e-06
    two_scale = jnp.max(jnp.abs(moment_two), axis=-1) + 1e-06
    one_code = (moment_one / one_scale[:, None]).astype(jnp.bfloat16)
    two_code = (moment_two / two_scale[:, None]).astype(jnp.bfloat16)
    return master_new, one_code, one_scale, two_code, two_scale


def reduce_pieces(piece, replicas):
    terms = {k: [piece(k)] for k in range(replicas)}
    total = lambda k: sum(t.astype(jnp.float32) for t in terms[k])
    for k in range(replicas - 1, 0, -1):
        sent = total(k).astype(jnp.bfloat16) if len(terms[k]) > 1 else terms[k][0]
        terms[k - low_bit(k)].append(swap(sent, low_bit(k)))
    return total(0)


def gather_pieces(own, replicas):
    held = {0: own}
    order = sorted(range(1, replicas), key=lambda k: (k.bit_count(), -k))
    for k in order:
        held[k] = swap(held[k - low_bit(k)], low_bit(k))
    return held, order


def per_device(grads, master, m_codes, m_scale, v_codes, v_scale):
    replicas = lax.axis_size("dp")
    owned, width = master.shape[1], master.shape[2]
    position = lax.axis_index("dp")
    rows = owned // CHUNKS
    parts = []
    weights = jnp.zeros((replicas * owned, width), jnp.bfloat16)
    for c in range(CHUNKS):
        start = lambda k: (position ^ k) * owned + c * rows
        piece = lambda k: lax.dynamic_slice(grads[0, 0], (start(k), 0), (rows, width))
        total = reduce_pieces(piece, replicas)
        mine = slice(c * rows, (c + 1) * rows)
        state = adam(
            total, replicas, master[0, mine], m_codes[0, mine], m_scale[0, mine],
            v_codes[0, mine], v_scale[0, mine],
        )
        parts.append(state)
        held, order = gather_pieces(state[0].astype(jnp.bfloat16), replicas)
        for k in [0] + order:
            weights = lax.dynamic_update_slice(weights, held[k], (start(k), 0))
    outs = [p[0] if CHUNKS == 1 else jnp.concatenate(p) for p in zip(*parts)]
    return tuple(o[None] for o in outs) + (weights[None],)


def solution(mesh):
    return jax.shard_map(
        per_device,
        mesh=mesh,
        in_specs=(
            P("dp", "mp", None, None),
            P("mp", "dp", None),
            P("mp", "dp", None),
            P("mp", "dp"),
            P("mp", "dp", None),
            P("mp", "dp"),
        ),
        out_specs=(
            P("mp", "dp", None),
            P("mp", "dp", None),
            P("mp", "dp"),
            P("mp", "dp", None),
            P("mp", "dp"),
            P("mp", None, None),
        ),
        check_vma=False,
    )
```

```python
import jax
import jax.numpy as jnp
from jax import lax
from jax.experimental import pallas as pl
from jax.experimental.pallas import tpu as pltpu
from jax.sharding import PartitionSpec as P

STEP = 8
PARTS = "ab"


def low_bit(k):
    return k & -k


def adam(total, replicas, master, m_codes, m_scale, v_codes, v_scale):
    grad_mean = total / replicas
    moment_one = 0.9 * m_codes.astype(jnp.float32) * m_scale[:, None] + 0.1 * grad_mean
    moment_two = (
        0.95 * v_codes.astype(jnp.float32) * v_scale[:, None] + 0.05 * grad_mean * grad_mean
    )
    first_fix = 1.0 - 0.9**STEP
    second_fix = 1.0 - 0.95**STEP
    master_new = master - 0.1 * (moment_one / first_fix) / (
        jnp.sqrt(moment_two / second_fix) + 1e-08
    )
    one_scale = jnp.max(jnp.abs(moment_one), axis=-1) + 1e-06
    two_scale = jnp.max(jnp.abs(moment_two), axis=-1) + 1e-06
    one_code = (moment_one / one_scale[:, None]).astype(jnp.bfloat16)
    two_code = (moment_two / two_scale[:, None]).astype(jnp.bfloat16)
    return master_new, one_code, two_code, one_scale, two_scale


TUNED = (
    "aF bF aN bN",
    "as6 bs6 as4 as2",
    "bs4 bs2",
    "au a4 a1 a2",
    "bu b4 b1 b2",
    "a5 a3 p0",
    "b6 b5 st a6",
    "b3 a7 b7",
    "p1 sc p2 p3",
)
PUTS = ("a0 a1 a2 a4",), ("b0 b1 b2", "a3 a5"), ("a6 a7", "b3 b4 b5"), ("b6 b7",)


def order_of(n):
    if n == 8:
        return " ".join(TUNED).split(), [" ".join(p).split() for p in PUTS]
    even = range(2, n, 2)
    far = [k for k in even[::-1] if k >= n // 2]
    near = [k for k in even[::-1] if k < n // 2]
    rest = sorted(range(2, n), key=lambda k: (k.bit_count(), k))
    steps = ["aF", "bF", "aN", "bN"]
    for c in "ab":
        steps += [f"{c}s{k}" for k in far] + [f"{c}s{k}" for k in near] + [c + "u"]
        steps += [c + "1"]
    steps += [f"{c}{k}" for k in rest for c in "ab"]
    blocks = [f"{c}{k}" for k in [0, 1] + rest for c in "ab"]
    return steps + ["st", "sc", "p0"], [blocks]


def sends(step):
    return step[-1] in "FN" or step[1:].lstrip("s").isdigit() and step[0] in "ab"


def swap(piece, bit):
    pairs = [(i, i ^ bit) for i in range(lax.axis_size("dp"))]
    return lax.ppermute(piece, "dp", pairs)


def place(owned, rows, spots, weights, pieces):
    def kernel(*refs):
        sources, target, sems = refs[: len(spots)], refs[-2], refs[-1]
        position = lax.axis_index("dp")
        copies = []
        for i, (k, at) in enumerate(spots):
            start = pl.multiple_of((position ^ k) * owned + at, rows)
            to = target.at[pl.ds(start, rows)]
            copies.append(pltpu.make_async_copy(sources[i], to, sems.at[i]))
        for copy in copies:
            copy.start()
        for copy in copies:
            copy.wait()

    operands = list(pieces)
    aliases = {}
    if not isinstance(weights, jax.ShapeDtypeStruct):
        aliases = {len(operands): 0}
        operands.append(weights)
    any_space = pl.BlockSpec(memory_space=pl.ANY)
    return pl.pallas_call(
        kernel,
        out_shape=jax.ShapeDtypeStruct(weights.shape, weights.dtype),
        in_specs=[any_space] * len(operands),
        out_specs=pl.BlockSpec(memory_space=pltpu.HBM),
        scratch_shapes=[pltpu.SemaphoreType.DMA((len(spots),))],
        input_output_aliases=aliases,
        compiler_params=pltpu.CompilerParams(vmem_limit_bytes=1 << 20),
    )(*operands)


def join(parts):
    count = len(parts[0])

    def kernel(*refs):
        sems = refs[-1]
        copies = []
        for i, blocks in enumerate(parts):
            target = refs[len(parts) * count + i]
            for j, block in enumerate(blocks):
                rows = block.shape[0]
                to = target.at[pl.ds(j * rows, rows)]
                copies.append(pltpu.make_async_copy(refs[i * count + j], to, sems.at[i, j]))
        for copy in copies:
            copy.start()
        for copy in copies:
            copy.wait()

    shapes = [
        jax.ShapeDtypeStruct((count * p[0].shape[0],) + p[0].shape[1:], p[0].dtype) for p in parts
    ]
    return pl.pallas_call(
        kernel,
        out_shape=shapes,
        in_specs=[pl.BlockSpec(memory_space=pl.ANY)] * (count * len(parts)),
        out_specs=[pl.BlockSpec(memory_space=pltpu.HBM)] * len(parts),
        scratch_shapes=[pltpu.SemaphoreType.DMA((len(parts), count))],
        compiler_params=pltpu.CompilerParams(vmem_limit_bytes=1 << 20),
    )(*[block for blocks in parts for block in blocks])


def per_device(grads, master, m_codes, m_scale, v_codes, v_scale):
    n = lax.axis_size("dp")
    owned, width = master.shape[1], master.shape[2]
    rows = owned // len(PARTS)
    first = {c: i * rows for i, c in enumerate(PARTS)}
    position = lax.axis_index("dp")
    top, low = position >> (n.bit_length() - 2), position & 1
    evens = range(0, n, 2)
    starts = [(position ^ k) * owned + first[c] for c in PARTS for k in evens]
    inside = [((position ^ k) >> 1 & (n // 4 - 1)) * rows for k in evens]
    source, *scalars = lax.optimization_barrier(
        (grads[0, 0], starts, inside, [top, 1 - top], 1 - low)
    )
    starts, inside, tops, mate = scalars
    start = dict(zip([(c, k) for c in PARTS for k in evens], starts))
    inside = dict(zip(evens, inside))
    terms = {key: [] for key in start}
    held, new = {}, {}
    state = [x[0] for x in (master, m_codes, v_codes, m_scale, v_scale)]
    weights = jax.ShapeDtypeStruct((n * owned, width), jnp.bfloat16)
    cut = lambda x, at, shape: lax.dynamic_slice(x, at, shape, allow_negative_indices=False)

    def total(c, k):
        own = cut(source, (start[c, k], 0), (rows, width))
        return sum((t().astype(jnp.float32) for t in terms[c, k]), own.astype(jnp.float32))

    steps, puts = order_of(n)
    for step in steps:
        c = step[0]
        if step[-1] in "FN":
            far = step[-1] == "F"
            view = source.reshape(2, n // 4, 2, owned, width)
            at = (tops[far], 0, mate, first[c], 0)
            sent = cut(view, at, (1, n // 4, 1, rows, width)).reshape(n // 4 * rows, width)
            sent, source = lax.optimization_barrier((sent, source))
        elif step[1] == "s" and step[2:].isdigit():
            k = int(step[2:])
            sent = total(c, k).astype(jnp.bfloat16)
            sent, source = lax.optimization_barrier((sent, source))
        elif step[-1] == "u":
            mine = slice(first[c], first[c] + rows)
            w, m, v, ms, vs = (x[mine] for x in state)
            new[c] = adam(total(c, 0), n, w, m, ms, v, vs)
            held[c, 0] = new[c][0].astype(jnp.bfloat16)
            held[c, 0], source, state = lax.optimization_barrier((held[c, 0], source, state))
        elif c == "p":
            blocks = [(x[0], int(x[1:])) for x in puts[int(step[1:])]]
            spots = [(k, first[d]) for d, k in blocks]
            weights = place(owned, rows, spots, weights, [held[x] for x in blocks])
        elif step == "st":
            joined = join([[new[d][i] for d in PARTS] for i in range(3)])
        elif step == "sc":
            one, two = (jnp.concatenate([new[d][i] for d in PARTS]) for i in (3, 4))
        if step[-1] in "FN":
            got = swap(sent, 1)
            for j in evens:
                if (j >= n // 2) == far:
                    terms[c, j].append(
                        lambda got=got, j=j: cut(got, (inside[j], 0), (rows, width))
                    )
        elif step[1] == "s" and step[2:].isdigit():
            got = swap(sent, low_bit(k))
            terms[c, k - low_bit(k)].append(lambda got=got: got)
        elif sends(step):
            k = int(step[1:])
            held[c, k] = swap(held[c, k - low_bit(k)], low_bit(k))
    return tuple(o[None] for o in (joined[0], joined[1], one, joined[2], two, weights))


def solution(mesh):
    return jax.shard_map(
        per_device,
        mesh=mesh,
        in_specs=(
            P("dp", "mp", None, None),
            P("mp", "dp", None),
            P("mp", "dp", None),
            P("mp", "dp"),
            P("mp", "dp", None),
            P("mp", "dp"),
        ),
        out_specs=(
            P("mp", "dp", None),
            P("mp", "dp", None),
            P("mp", "dp"),
            P("mp", "dp", None),
            P("mp", "dp"),
            P("mp", None, None),
        ),
        check_vma=False,
    )
```

```python
import math

import jax
import jax.numpy as jnp
from jax import lax
from jax.experimental import pallas as pl
from jax.experimental.pallas import tpu as pltpu
from jax.sharding import PartitionSpec as P

STEP = 8
SHARES = {"a": 9, "b": 7}


def low_bit(k):
    return k & -k


def adam(total, replicas, master, m_codes, m_scale, v_codes, v_scale):
    grad_mean = total / replicas
    moment_one = 0.9 * m_codes.astype(jnp.float32) * m_scale[:, None] + 0.1 * grad_mean
    moment_two = (
        0.95 * v_codes.astype(jnp.float32) * v_scale[:, None] + 0.05 * grad_mean * grad_mean
    )
    first_fix = 1.0 - 0.9**STEP
    second_fix = 1.0 - 0.95**STEP
    master_new = master - 0.1 * (moment_one / first_fix) / (
        jnp.sqrt(moment_two / second_fix) + 1e-08
    )
    one_scale = jnp.max(jnp.abs(moment_one), axis=-1) + 1e-06
    two_scale = jnp.max(jnp.abs(moment_two), axis=-1) + 1e-06
    one_code = (moment_one / one_scale[:, None]).astype(jnp.bfloat16)
    two_code = (moment_two / two_scale[:, None]).astype(jnp.bfloat16)
    return master_new, one_code, two_code, one_scale, two_scale


TUNED = (
    "ar75 ar32 br75 as6",
    "br31 bs6 as4 as1",
    "bs2 bs4 au a2",
    "a1 a4 bu b2",
    "b1 b4 a3 a5",
    "a6 b3 sc p0",
    "b6 b5 a7 p1",
    "b7 p2 st p3",
)
PUTS = (
    ("a0 a1 a2 a4", "b0",),
    ("b1 b2 b4 a3",),
    ("a5 a6 b3 b6", "b5",),
    ("a7 b7",),
)
GROUPS = ()
TURNS = {"ar": {3: 2}, "br": {}, "a": {7: 2}, "b": {}}


def order_of(n):
    if n == 8:
        steps = " ".join(TUNED).split()
        raw = {s: [int(k) for k in s[2:]] for s in steps if s[1] == "r"}
        groups = {f"g{i}": g.split() for i, g in enumerate(GROUPS)}
        return steps, [" ".join(p).split() for p in PUTS], raw, TURNS, groups
    odd = range(n - 1, 0, -2)
    even = range(n - 2, 0, -2)
    halves = [k for k in odd if k > n // 2], [k for k in odd if k < n // 2]
    raw = {f"{c}r{i}": halves[i] for i in range(2) for c in "ab"}
    rest = sorted(range(2, n), key=lambda k: (k.bit_count(), k))
    steps = list(raw)
    for c in "ab":
        steps += [f"{c}s{k}" for k in even] + [c + "u", c + "1"]
    steps += [f"{c}{k}" for k in rest for c in "ab"]
    blocks = [f"{c}{k}" for k in [0, 1] + rest for c in "ab"]
    return steps + ["st", "sc", "p0"], [blocks], raw, {x: {} for x in TURNS}, {}


def sends(step):
    return step[0] in "abg" and step[1:].lstrip("rs").isdigit()


def swap(piece, bit):
    pairs = [(i, i ^ bit) for i in range(lax.axis_size("dp"))]
    return lax.ppermute(piece, "dp", pairs)


def place(owned, spots, weights, pieces):
    def kernel(*refs):
        sources, target, sems = refs[: len(spots)], refs[-2], refs[-1]
        position = lax.axis_index("dp")
        copies = []
        for i, (k, at, rows) in enumerate(spots):
            start = pl.multiple_of((position ^ k) * owned + at, math.gcd(owned, at))
            source = sources[i].at[pl.ds(pieces[i][1], rows)]
            to = target.at[pl.ds(start, rows)]
            copies.append(pltpu.make_async_copy(source, to, sems.at[i]))
        for copy in copies:
            copy.start()
        for copy in copies:
            copy.wait()

    operands = [piece for piece, _ in pieces]
    aliases = {}
    if not isinstance(weights, jax.ShapeDtypeStruct):
        aliases = {len(operands): 0}
        operands.append(weights)
    any_space = pl.BlockSpec(memory_space=pl.ANY)
    return pl.pallas_call(
        kernel,
        out_shape=jax.ShapeDtypeStruct(weights.shape, weights.dtype),
        in_specs=[any_space] * len(operands),
        out_specs=pl.BlockSpec(memory_space=pltpu.HBM),
        scratch_shapes=[pltpu.SemaphoreType.DMA((len(spots),))],
        input_output_aliases=aliases,
        compiler_params=pltpu.CompilerParams(vmem_limit_bytes=1 << 20),
    )(*operands)


def join(parts):
    count = len(parts[0])

    def kernel(*refs):
        sems = refs[-1]
        copies = []
        for i, blocks in enumerate(parts):
            target = refs[len(parts) * count + i]
            at = 0
            for j, block in enumerate(blocks):
                rows = block.shape[0]
                to = target.at[pl.ds(at, rows)]
                at += rows
                copies.append(pltpu.make_async_copy(refs[i * count + j], to, sems.at[i, j]))
        for copy in copies:
            copy.start()
        for copy in copies:
            copy.wait()

    shapes = [
        jax.ShapeDtypeStruct((sum(b.shape[0] for b in p),) + p[0].shape[1:], p[0].dtype)
        for p in parts
    ]
    return pl.pallas_call(
        kernel,
        out_shape=shapes,
        in_specs=[pl.BlockSpec(memory_space=pl.ANY)] * (count * len(parts)),
        out_specs=[pl.BlockSpec(memory_space=pltpu.HBM)] * len(parts),
        scratch_shapes=[pltpu.SemaphoreType.DMA((len(parts), count))],
        compiler_params=pltpu.CompilerParams(vmem_limit_bytes=1 << 20),
    )(*[block for blocks in parts for block in blocks])


def per_device(grads, master, m_codes, m_scale, v_codes, v_scale):
    n = lax.axis_size("dp")
    digits = n.bit_length() - 1
    owned, width = master.shape[1], master.shape[2]
    rows, first, at = {}, {}, 0
    for c, share in SHARES.items():
        first[c], rows[c] = at, owned * share // sum(SHARES.values())
        at += rows[c]
    position = lax.axis_index("dp")
    steps, puts, raw, turns, groups = order_of(n)
    by = lambda kind, k: turns[kind].get(k, low_bit(k))
    bits = [position >> i & 1 for i in range(digits)]
    scalars = {}
    for i in range(digits):
        scalars["bit", i, 0], scalars["bit", i, 1] = bits[i], 1 - bits[i]
    free = {s: [i for i in range(digits) if len({k >> i & 1 for k in raw[s]}) > 1] for s in raw}
    kept = [(c, k) for c in SHARES for k in range(n) if not any(k in raw[s] for s in raw if s[0] == c)]
    for c, k in kept:
        scalars["own", c, k] = (position ^ k) * owned + first[c]
    for s in raw:
        for k in raw[s]:
            to = k ^ by(s[:2], k)
            index = sum((bits[i] ^ (to >> i & 1)) << j for j, i in enumerate(free[s]))
            scalars["got", s, k] = index * rows[s[0]]
    source, scalars = lax.optimization_barrier((grads[0, 0], scalars))
    terms = {key: [] for key in kept}
    held, new = {}, {}
    state = [x[0] for x in (master, m_codes, v_codes, m_scale, v_scale)]
    weights = jax.ShapeDtypeStruct((n * owned, width), jnp.bfloat16)
    cut = lambda x, at, shape: lax.dynamic_slice(x, at, shape, allow_negative_indices=False)

    def total(c, k):
        own = cut(source, (scalars["own", c, k], 0), (rows[c], width))
        return sum((t().astype(jnp.float32) for t in terms[c, k]), own.astype(jnp.float32))

    def block(c, k):
        whole, at = held[c, k]
        return lax.slice_in_dim(whole, at, at + rows[c])

    for step in steps:
        c = step[0]
        if step in raw:
            k, spread = raw[step][0], free[step]
            order = range(digits - 1, -1, -1)
            at = [0 if i in spread else scalars["bit", i, k >> i & 1] for i in order]
            size = [2 if i in spread else 1 for i in order]
            view = source.reshape([2] * digits + [owned, width])
            sent = cut(view, (*at, first[c], 0), (*size, rows[c], width))
            sent = sent.reshape(len(raw[step]) * rows[c], width)
            sent, source = lax.optimization_barrier((sent, source))
        elif step[1] == "s" and step[2:].isdigit():
            k = int(step[2:])
            sent = total(c, k).astype(jnp.bfloat16)
            sent, source = lax.optimization_barrier((sent, source))
        elif step[-1] == "u":
            mine = slice(first[c], first[c] + rows[c])
            w, m, v, ms, vs = (x[mine] for x in state)
            new[c] = adam(total(c, 0), n, w, m, ms, v, vs)
            mine = new[c][0].astype(jnp.bfloat16)
            mine, source, state = lax.optimization_barrier((mine, source, state))
            held[c, 0] = mine, 0
        elif c == "p":
            blocks = [(x[0], int(x[1:])) for x in puts[int(step[1:])]]
            spots = [(k, first[d], rows[d]) for d, k in blocks]
            weights = place(owned, spots, weights, [held[x] for x in blocks])
        elif step in groups:
            blocks = [(x[0], int(x[1:])) for x in groups[step]]
            bit = by(*blocks[0])
            ends = [sum(rows[d] for d, _ in blocks[:i]) for i in range(len(blocks) + 1)]
            sent = jnp.zeros((ends[-1], width), jnp.bfloat16)
            sent = lax.optimization_barrier(sent)
            for (d, k), at in zip(blocks, ends):
                sent = lax.dynamic_update_slice(sent, block(d, k ^ bit), (at, 0))
        elif step == "st":
            joined = join([[new[d][i] for d in SHARES] for i in range(3)])
        elif step == "sc":
            one, two = (jnp.concatenate([new[d][i] for d in SHARES]) for i in (3, 4))
        if step in raw:
            got = swap(sent, by(step[:2], k))
            for k in raw[step]:
                terms[c, k ^ by(step[:2], k)].append(
                    lambda got=got, c=c, at=scalars["got", step, k]: cut(
                        got, (at, 0), (rows[c], width)
                    )
                )
        elif step[1] == "s" and step[2:].isdigit():
            bit = by(c + "r", k)
            got = swap(sent, bit)
            terms[c, k ^ bit].append(lambda got=got: got)
        elif step in groups:
            got = swap(sent, bit)
            held.update({key: (got, at) for key, at in zip(blocks, ends)})
        elif sends(step):
            k = int(step[1:])
            bit = by(c, k)
            held[c, k] = swap(block(c, k ^ bit), bit), 0
    return tuple(o[None] for o in (joined[0], joined[1], one, joined[2], two, weights))


def solution(mesh):
    return jax.shard_map(
        per_device,
        mesh=mesh,
        in_specs=(
            P("dp", "mp", None, None),
            P("mp", "dp", None),
            P("mp", "dp", None),
            P("mp", "dp"),
            P("mp", "dp", None),
            P("mp", "dp"),
        ),
        out_specs=(
            P("mp", "dp", None),
            P("mp", "dp", None),
            P("mp", "dp"),
            P("mp", "dp", None),
            P("mp", "dp"),
            P("mp", None, None),
        ),
        check_vma=False,
    )
```

```python
import math

import jax
import jax.numpy as jnp
from jax import lax
from jax.experimental import pallas as pl
from jax.experimental.pallas import tpu as pltpu
from jax.sharding import PartitionSpec as P

STEP = 8
SHARES = {"a": 17, "b": 15}


def low_bit(k):
    return k & -k


def moments(total, replicas, m_codes, m_scale, v_codes, v_scale):
    grad_mean = total / replicas
    moment_one = 0.9 * m_codes.astype(jnp.float32) * m_scale[:, None] + 0.1 * grad_mean
    moment_two = (
        0.95 * v_codes.astype(jnp.float32) * v_scale[:, None] + 0.05 * grad_mean * grad_mean
    )
    return moment_one, moment_two


def stepped(master, moment_one, moment_two):
    first_fix = 1.0 - 0.9**STEP
    second_fix = 1.0 - 0.95**STEP
    return master - 0.1 * (moment_one / first_fix) / (
        jnp.sqrt(moment_two / second_fix) + 1e-08
    )


def state_code(values):
    scale = jnp.max(jnp.abs(values), axis=-1) + 1e-06
    return (values / scale[:, None]).astype(jnp.bfloat16), scale


TUNED = (
    "ar75 ar32 br75 as6",
    "br31 bs6 as4 as1",
    "bs2 bs4 au a2",
    "a1 a4 bu b2",
    "b1 b4 a3 a5",
    "a6 b3 p0",
    "b6 b5 a7 p1",
    "b7 p2 st p3",
)
PUTS = (
    ("a0 a1 a2 a4", "b0",),
    ("b1 b2 b4 a3",),
    ("a5 a6 b3 b6", "b5",),
    ("a7 b7",),
)
GROUPS = ()
TURNS = {"ar": {3: 2}, "br": {}, "a": {7: 2}, "b": {}}


def order_of(n):
    if n == 8:
        steps = " ".join(TUNED).split()
        raw = {s: [int(k) for k in s[2:]] for s in steps if s[1] == "r"}
        groups = {f"g{i}": g.split() for i, g in enumerate(GROUPS)}
        return steps, [" ".join(p).split() for p in PUTS], raw, TURNS, groups
    odd = range(n - 1, 0, -2)
    even = range(n - 2, 0, -2)
    halves = [k for k in odd if k > n // 2], [k for k in odd if k < n // 2]
    raw = {f"{c}r{i}": halves[i] for i in range(2) for c in "ab"}
    rest = sorted(range(2, n), key=lambda k: (k.bit_count(), k))
    steps = list(raw)
    for c in "ab":
        steps += [f"{c}s{k}" for k in even] + [c + "u", c + "1"]
    steps += [f"{c}{k}" for k in rest for c in "ab"]
    blocks = [f"{c}{k}" for k in [0, 1] + rest for c in "ab"]
    return steps + ["st", "p0"], [blocks], raw, {x: {} for x in TURNS}, {}


def sends(step):
    return step[0] in "abg" and step[1:].lstrip("rs").isdigit()


def swap(piece, bit):
    pairs = [(i, i ^ bit) for i in range(lax.axis_size("dp"))]
    return lax.ppermute(piece, "dp", pairs)


def place(owned, spots, weights, pieces):
    def kernel(*refs):
        sources, target, sems = refs[: len(spots)], refs[-2], refs[-1]
        position = lax.axis_index("dp")
        copies = []
        for i, (k, at, rows) in enumerate(spots):
            start = pl.multiple_of((position ^ k) * owned + at, math.gcd(owned, at))
            source = sources[i].at[pl.ds(pieces[i][1], rows)]
            to = target.at[pl.ds(start, rows)]
            copies.append(pltpu.make_async_copy(source, to, sems.at[i]))
        for copy in copies:
            copy.start()
        for copy in copies:
            copy.wait()

    operands = [piece for piece, _ in pieces]
    aliases = {}
    if not isinstance(weights, jax.ShapeDtypeStruct):
        aliases = {len(operands): 0}
        operands.append(weights)
    any_space = pl.BlockSpec(memory_space=pl.ANY)
    return pl.pallas_call(
        kernel,
        out_shape=jax.ShapeDtypeStruct(weights.shape, weights.dtype),
        in_specs=[any_space] * len(operands),
        out_specs=pl.BlockSpec(memory_space=pltpu.HBM),
        scratch_shapes=[pltpu.SemaphoreType.DMA((len(spots),))],
        input_output_aliases=aliases,
        compiler_params=pltpu.CompilerParams(vmem_limit_bytes=1 << 20),
    )(*operands)


def per_device(grads, master, m_codes, m_scale, v_codes, v_scale):
    n = lax.axis_size("dp")
    digits = n.bit_length() - 1
    owned, width = master.shape[1], master.shape[2]
    rows, first, at = {}, {}, 0
    for c, share in SHARES.items():
        first[c], rows[c] = at, owned * share // sum(SHARES.values())
        at += rows[c]
    position = lax.axis_index("dp")
    steps, puts, raw, turns, groups = order_of(n)
    by = lambda kind, k: turns[kind].get(k, low_bit(k))
    bits = [position >> i & 1 for i in range(digits)]
    scalars = {}
    for i in range(digits):
        scalars["bit", i, 0], scalars["bit", i, 1] = bits[i], 1 - bits[i]
    free = {s: [i for i in range(digits) if len({k >> i & 1 for k in raw[s]}) > 1] for s in raw}
    kept = [(c, k) for c in SHARES for k in range(n) if not any(k in raw[s] for s in raw if s[0] == c)]
    for c, k in kept:
        scalars["own", c, k] = (position ^ k) * owned + first[c]
    for s in raw:
        for k in raw[s]:
            to = k ^ by(s[:2], k)
            index = sum((bits[i] ^ (to >> i & 1)) << j for j, i in enumerate(free[s]))
            scalars["got", s, k] = index * rows[s[0]]
    source, scalars = lax.optimization_barrier((grads[0, 0], scalars))
    terms = {key: [] for key in kept}
    held = {}
    sums = lax.optimization_barrier(jnp.zeros((owned, width), jnp.float32))
    state = [x[0] for x in (master, m_codes, v_codes, m_scale, v_scale)]
    weights = jax.ShapeDtypeStruct((n * owned, width), jnp.bfloat16)
    cut = lambda x, at, shape: lax.dynamic_slice(x, at, shape, allow_negative_indices=False)

    def total(c, k):
        own = cut(source, (scalars["own", c, k], 0), (rows[c], width))
        return sum((t().astype(jnp.float32) for t in terms[c, k]), own.astype(jnp.float32))

    def block(c, k):
        whole, at = held[c, k]
        return lax.slice_in_dim(whole, at, at + rows[c])

    for step in steps:
        c = step[0]
        if step in raw:
            k, spread = raw[step][0], free[step]
            order = range(digits - 1, -1, -1)
            at = [0 if i in spread else scalars["bit", i, k >> i & 1] for i in order]
            size = [2 if i in spread else 1 for i in order]
            view = source.reshape([2] * digits + [owned, width])
            sent = cut(view, (*at, first[c], 0), (*size, rows[c], width))
            sent = sent.reshape(len(raw[step]) * rows[c], width)
            sent, source = lax.optimization_barrier((sent, source))
        elif step[1] == "s" and step[2:].isdigit():
            k = int(step[2:])
            sent = total(c, k).astype(jnp.bfloat16)
            sent, source = lax.optimization_barrier((sent, source))
        elif step[-1] == "u":
            mine = slice(first[c], first[c] + rows[c])
            summed = total(c, 0)
            w, m, v, ms, vs = (x[mine] for x in state)
            mine = stepped(w, *moments(summed, n, m, ms, v, vs)).astype(jnp.bfloat16)
            sums = lax.dynamic_update_slice(sums, summed, (first[c], 0))
            mine, sums, source, state = lax.optimization_barrier((mine, sums, source, state))
            held[c, 0] = mine, 0
        elif c == "p":
            blocks = [(x[0], int(x[1:])) for x in puts[int(step[1:])]]
            spots = [(k, first[d], rows[d]) for d, k in blocks]
            weights = place(owned, spots, weights, [held[x] for x in blocks])
        elif step in groups:
            blocks = [(x[0], int(x[1:])) for x in groups[step]]
            bit = by(*blocks[0])
            ends = [sum(rows[d] for d, _ in blocks[:i]) for i in range(len(blocks) + 1)]
            sent = jnp.zeros((ends[-1], width), jnp.bfloat16)
            sent = lax.optimization_barrier(sent)
            for (d, k), at in zip(blocks, ends):
                sent = lax.dynamic_update_slice(sent, block(d, k ^ bit), (at, 0))
        elif step == "st":
            w, m, v, ms, vs = state
            one, two = moments(sums, n, m, ms, v, vs)
            master_new = stepped(w, one, two)
            (m_new, m_top), (v_new, v_top) = state_code(one), state_code(two)
        if step in raw:
            got = swap(sent, by(step[:2], k))
            for k in raw[step]:
                terms[c, k ^ by(step[:2], k)].append(
                    lambda got=got, c=c, at=scalars["got", step, k]: cut(
                        got, (at, 0), (rows[c], width)
                    )
                )
        elif step[1] == "s" and step[2:].isdigit():
            bit = by(c + "r", k)
            got = swap(sent, bit)
            terms[c, k ^ bit].append(lambda got=got: got)
        elif step in groups:
            got = swap(sent, bit)
            held.update({key: (got, at) for key, at in zip(blocks, ends)})
        elif sends(step):
            k = int(step[1:])
            bit = by(c, k)
            held[c, k] = swap(block(c, k ^ bit), bit), 0
    return tuple(o[None] for o in (master_new, m_new, m_top, v_new, v_top, weights))


def solution(mesh):
    return jax.shard_map(
        per_device,
        mesh=mesh,
        in_specs=(
            P("dp", "mp", None, None),
            P("mp", "dp", None),
            P("mp", "dp", None),
            P("mp", "dp"),
            P("mp", "dp", None),
            P("mp", "dp"),
        ),
        out_specs=(
            P("mp", "dp", None),
            P("mp", "dp", None),
            P("mp", "dp"),
            P("mp", "dp", None),
            P("mp", "dp"),
            P("mp", None, None),
        ),
        check_vma=False,
    )
```

```python
import math

import jax
import jax.numpy as jnp
from jax import lax
from jax.experimental import pallas as pl
from jax.experimental.pallas import tpu as pltpu
from jax.sharding import PartitionSpec as P

STEP = 8
SHARES = {"a": 17, "b": 15}


def low_bit(k):
    return k & -k


def moments(total, replicas, m_codes, m_scale, v_codes, v_scale):
    grad_mean = total / replicas
    moment_one = 0.9 * m_codes.astype(jnp.float32) * m_scale[:, None] + 0.1 * grad_mean
    moment_two = (
        0.95 * v_codes.astype(jnp.float32) * v_scale[:, None] + 0.05 * grad_mean * grad_mean
    )
    return moment_one, moment_two


def stepped(master, moment_one, moment_two):
    first_fix = 1.0 - 0.9**STEP
    second_fix = 1.0 - 0.95**STEP
    return master - 0.1 * (moment_one / first_fix) / (
        jnp.sqrt(moment_two / second_fix) + 1e-08
    )


def state_code(values):
    scale = jnp.max(jnp.abs(values), axis=-1) + 1e-06
    return (values / scale[:, None]).astype(jnp.bfloat16), scale


TUNED = (
    "ar75 ar32 br75 ao6",
    "as6 br31 bs6 as4",
    "as1 bs2 bs4 au",
    "a1 a2 a4 bu",
    "b2 b1 b4 a3",
    "a5 a6 p0 b3",
    "b6 b5 a7 p1",
    "b7 p2 st p3",
)
PUTS = (
    ("a0 a1 a2 a4", "b0",),
    ("b1 b2 b4 a3",),
    ("a5 a6 b3 b6", "b5",),
    ("a7 b7",),
)
GROUPS = ()
TURNS = {"ar": {3: 2}, "br": {}, "a": {7: 2}, "b": {}}


def order_of(n):
    if n == 8:
        steps = " ".join(TUNED).split()
        raw = {s: [int(k) for k in s[2:]] for s in steps if s[1] == "r"}
        groups = {f"g{i}": g.split() for i, g in enumerate(GROUPS)}
        return steps, [" ".join(p).split() for p in PUTS], raw, TURNS, groups
    odd = range(n - 1, 0, -2)
    even = range(n - 2, 0, -2)
    halves = [k for k in odd if k > n // 2], [k for k in odd if k < n // 2]
    raw = {f"{c}r{i}": halves[i] for i in range(2) for c in "ab"}
    rest = sorted(range(2, n), key=lambda k: (k.bit_count(), k))
    steps = list(raw)
    for c in "ab":
        steps += [f"{c}s{k}" for k in even] + [c + "u", c + "1"]
    steps += [f"{c}{k}" for k in rest for c in "ab"]
    blocks = [f"{c}{k}" for k in [0, 1] + rest for c in "ab"]
    return steps + ["st", "p0"], [blocks], raw, {x: {} for x in TURNS}, {}


def sends(step):
    return step[0] in "abg" and step[1:].lstrip("rs").isdigit()


def swap(piece, bit):
    pairs = [(i, i ^ bit) for i in range(lax.axis_size("dp"))]
    return lax.ppermute(piece, "dp", pairs)


def place(owned, spots, weights, pieces):
    def kernel(*refs):
        sources, target, sems = refs[: len(spots)], refs[-2], refs[-1]
        position = lax.axis_index("dp")
        copies = []
        for i, (k, at, rows) in enumerate(spots):
            start = pl.multiple_of((position ^ k) * owned + at, math.gcd(owned, at))
            source = sources[i].at[pl.ds(pieces[i][1], rows)]
            to = target.at[pl.ds(start, rows)]
            copies.append(pltpu.make_async_copy(source, to, sems.at[i]))
        for copy in copies:
            copy.start()
        for copy in copies:
            copy.wait()

    operands = [piece for piece, _ in pieces]
    aliases = {}
    if not isinstance(weights, jax.ShapeDtypeStruct):
        aliases = {len(operands): 0}
        operands.append(weights)
    any_space = pl.BlockSpec(memory_space=pl.ANY)
    return pl.pallas_call(
        kernel,
        out_shape=jax.ShapeDtypeStruct(weights.shape, weights.dtype),
        in_specs=[any_space] * len(operands),
        out_specs=pl.BlockSpec(memory_space=pltpu.HBM),
        scratch_shapes=[pltpu.SemaphoreType.DMA((len(spots),))],
        input_output_aliases=aliases,
        compiler_params=pltpu.CompilerParams(vmem_limit_bytes=1 << 20),
    )(*operands)


def per_device(grads, master, m_codes, m_scale, v_codes, v_scale):
    n = lax.axis_size("dp")
    digits = n.bit_length() - 1
    owned, width = master.shape[1], master.shape[2]
    rows, first, at = {}, {}, 0
    for c, share in SHARES.items():
        first[c], rows[c] = at, owned * share // sum(SHARES.values())
        at += rows[c]
    position = lax.axis_index("dp")
    steps, puts, raw, turns, groups = order_of(n)
    by = lambda kind, k: turns[kind].get(k, low_bit(k))
    bits = [position >> i & 1 for i in range(digits)]
    scalars = {}
    for i in range(digits):
        scalars["bit", i, 0], scalars["bit", i, 1] = bits[i], 1 - bits[i]
    free = {s: [i for i in range(digits) if len({k >> i & 1 for k in raw[s]}) > 1] for s in raw}
    kept = [(c, k) for c in SHARES for k in range(n) if not any(k in raw[s] for s in raw if s[0] == c)]
    for c, k in kept:
        scalars["own", c, k] = (position ^ k) * owned + first[c]
    for s in raw:
        for k in raw[s]:
            to = k ^ by(s[:2], k)
            index = sum((bits[i] ^ (to >> i & 1)) << j for j, i in enumerate(free[s]))
            scalars["got", s, k] = index * rows[s[0]]
    source, scalars = lax.optimization_barrier((grads[0, 0], scalars))
    terms = {key: [] for key in kept}
    held, copied = {}, {}
    sums = lax.optimization_barrier(jnp.zeros((owned, width), jnp.float32))
    state = [x[0] for x in (master, m_codes, v_codes, m_scale, v_scale)]
    weights = jax.ShapeDtypeStruct((n * owned, width), jnp.bfloat16)
    cut = lambda x, at, shape: lax.dynamic_slice(x, at, shape, allow_negative_indices=False)

    def own_piece(c, k):
        return cut(source, (scalars["own", c, k], 0), (rows[c], width))

    def total(c, k):
        own = copied[c, k] if (c, k) in copied else own_piece(c, k)
        return sum((t().astype(jnp.float32) for t in terms[c, k]), own.astype(jnp.float32))

    def block(c, k):
        whole, at = held[c, k]
        return lax.slice_in_dim(whole, at, at + rows[c])

    for step in steps:
        c = step[0]
        if step in raw:
            k, spread = raw[step][0], free[step]
            order = range(digits - 1, -1, -1)
            at = [0 if i in spread else scalars["bit", i, k >> i & 1] for i in order]
            size = [2 if i in spread else 1 for i in order]
            view = source.reshape([2] * digits + [owned, width])
            sent = cut(view, (*at, first[c], 0), (*size, rows[c], width))
            sent = sent.reshape(len(raw[step]) * rows[c], width)
            sent, source = lax.optimization_barrier((sent, source))
        elif step[1] == "s" and step[2:].isdigit():
            k = int(step[2:])
            sent = total(c, k).astype(jnp.bfloat16)
            sent, source = lax.optimization_barrier((sent, source))
        elif step[1] == "o":
            own, source = lax.optimization_barrier((own_piece(c, int(step[2:])), source))
            copied[c, int(step[2:])] = own
        elif step[-1] == "u":
            mine = slice(first[c], first[c] + rows[c])
            summed = total(c, 0)
            w, m, v, ms, vs = (x[mine] for x in state)
            mine = stepped(w, *moments(summed, n, m, ms, v, vs)).astype(jnp.bfloat16)
            sums = lax.dynamic_update_slice(sums, summed, (first[c], 0))
            mine, sums, source, state = lax.optimization_barrier((mine, sums, source, state))
            held[c, 0] = mine, 0
        elif c == "p":
            blocks = [(x[0], int(x[1:])) for x in puts[int(step[1:])]]
            spots = [(k, first[d], rows[d]) for d, k in blocks]
            weights = place(owned, spots, weights, [held[x] for x in blocks])
        elif step in groups:
            blocks = [(x[0], int(x[1:])) for x in groups[step]]
            bit = by(*blocks[0])
            ends = [sum(rows[d] for d, _ in blocks[:i]) for i in range(len(blocks) + 1)]
            sent = jnp.zeros((ends[-1], width), jnp.bfloat16)
            sent = lax.optimization_barrier(sent)
            for (d, k), at in zip(blocks, ends):
                sent = lax.dynamic_update_slice(sent, block(d, k ^ bit), (at, 0))
        elif step == "st":
            w, m, v, ms, vs = state
            one, two = moments(sums, n, m, ms, v, vs)
            master_new = stepped(w, one, two)
            (m_new, m_top), (v_new, v_top) = state_code(one), state_code(two)
        if step in raw:
            got = swap(sent, by(step[:2], k))
            for k in raw[step]:
                terms[c, k ^ by(step[:2], k)].append(
                    lambda got=got, c=c, at=scalars["got", step, k]: cut(
                        got, (at, 0), (rows[c], width)
                    )
                )
        elif step[1] == "s" and step[2:].isdigit():
            bit = by(c + "r", k)
            got = swap(sent, bit)
            terms[c, k ^ bit].append(lambda got=got: got)
        elif step in groups:
            got = swap(sent, bit)
            held.update({key: (got, at) for key, at in zip(blocks, ends)})
        elif sends(step):
            k = int(step[1:])
            bit = by(c, k)
            held[c, k] = swap(block(c, k ^ bit), bit), 0
    return tuple(o[None] for o in (master_new, m_new, m_top, v_new, v_top, weights))


def solution(mesh):
    return jax.shard_map(
        per_device,
        mesh=mesh,
        in_specs=(
            P("dp", "mp", None, None),
            P("mp", "dp", None),
            P("mp", "dp", None),
            P("mp", "dp"),
            P("mp", "dp", None),
            P("mp", "dp"),
        ),
        out_specs=(
            P("mp", "dp", None),
            P("mp", "dp", None),
            P("mp", "dp"),
            P("mp", "dp", None),
            P("mp", "dp"),
            P("mp", None, None),
        ),
        check_vma=False,
    )
```

```python
import math

import jax
import jax.numpy as jnp
from jax import lax
from jax.experimental import pallas as pl
from jax.experimental.pallas import tpu as pltpu
from jax.sharding import PartitionSpec as P

STEP = 8
SHARES = {"a": 17, "b": 15}


def low_bit(k):
    return k & -k


def moments(total, replicas, m_codes, m_scale, v_codes, v_scale):
    grad_mean = total / replicas
    moment_one = 0.9 * m_codes.astype(jnp.float32) * m_scale[:, None] + 0.1 * grad_mean
    moment_two = (
        0.95 * v_codes.astype(jnp.float32) * v_scale[:, None] + 0.05 * grad_mean * grad_mean
    )
    return moment_one, moment_two


def stepped(master, moment_one, moment_two):
    first_fix = 1.0 - 0.9**STEP
    second_fix = 1.0 - 0.95**STEP
    return master - 0.1 * (moment_one / first_fix) / (
        jnp.sqrt(moment_two / second_fix) + 1e-08
    )


def state_code(values):
    scale = jnp.max(jnp.abs(values), axis=-1) + 1e-06
    return (values / scale[:, None]).astype(jnp.bfloat16), scale


TUNED = (
    "ar75 ar32 br75 ao6",
    "as6 br31 bs6 as4",
    "as1 bs2 bs4 au",
    "a1 a2 a4 bu",
    "b2 b1 b4 a3",
    "a5 a6 p0 b3",
    "b6 b5 a7 b7",
    "p1 st p2",
)
PUTS = (
    ("a0 a1 a2 a4", "b0",),
    ("b1 b2 b4 a3", "a5 a6 b3 b6", "b5",),
    ("a7 b7",),
)
GROUPS = ()
TURNS = {"ar": {3: 2}, "br": {}, "a": {7: 2}, "b": {}}


def order_of(n):
    if n == 8:
        steps = " ".join(TUNED).split()
        raw = {s: [int(k) for k in s[2:]] for s in steps if s[1] == "r"}
        groups = {f"g{i}": g.split() for i, g in enumerate(GROUPS)}
        return steps, [" ".join(p).split() for p in PUTS], raw, TURNS, groups
    odd = range(n - 1, 0, -2)
    even = range(n - 2, 0, -2)
    halves = [k for k in odd if k > n // 2], [k for k in odd if k < n // 2]
    raw = {f"{c}r{i}": halves[i] for i in range(2) for c in "ab"}
    rest = sorted(range(2, n), key=lambda k: (k.bit_count(), k))
    steps = list(raw)
    for c in "ab":
        steps += [f"{c}s{k}" for k in even] + [c + "u", c + "1"]
    steps += [f"{c}{k}" for k in rest for c in "ab"]
    blocks = [f"{c}{k}" for k in [0, 1] + rest for c in "ab"]
    return steps + ["st", "p0"], [blocks], raw, {x: {} for x in TURNS}, {}


def sends(step):
    return step[0] in "abg" and step[1:].lstrip("rs").isdigit()


def swap(piece, bit):
    pairs = [(i, i ^ bit) for i in range(lax.axis_size("dp"))]
    return lax.ppermute(piece, "dp", pairs)


def place(owned, spots, weights, pieces):
    def kernel(*refs):
        sources, target, sems = refs[: len(spots)], refs[-2], refs[-1]
        position = lax.axis_index("dp")
        copies = []
        for i, (k, at, rows) in enumerate(spots):
            start = pl.multiple_of((position ^ k) * owned + at, math.gcd(owned, at))
            source = sources[i].at[pl.ds(pieces[i][1], rows)]
            to = target.at[pl.ds(start, rows)]
            copies.append(pltpu.make_async_copy(source, to, sems.at[i]))
        for copy in copies:
            copy.start()
        for copy in copies:
            copy.wait()

    operands = [piece for piece, _ in pieces]
    aliases = {}
    if not isinstance(weights, jax.ShapeDtypeStruct):
        aliases = {len(operands): 0}
        operands.append(weights)
    any_space = pl.BlockSpec(memory_space=pl.ANY)
    return pl.pallas_call(
        kernel,
        out_shape=jax.ShapeDtypeStruct(weights.shape, weights.dtype),
        in_specs=[any_space] * len(operands),
        out_specs=pl.BlockSpec(memory_space=pltpu.HBM),
        scratch_shapes=[pltpu.SemaphoreType.DMA((len(spots),))],
        input_output_aliases=aliases,
        compiler_params=pltpu.CompilerParams(vmem_limit_bytes=1 << 20),
    )(*operands)


def per_device(grads, master, m_codes, m_scale, v_codes, v_scale):
    n = lax.axis_size("dp")
    digits = n.bit_length() - 1
    owned, width = master.shape[1], master.shape[2]
    rows, first, at = {}, {}, 0
    for c, share in SHARES.items():
        first[c], rows[c] = at, owned * share // sum(SHARES.values())
        at += rows[c]
    position = lax.axis_index("dp")
    steps, puts, raw, turns, groups = order_of(n)
    by = lambda kind, k: turns[kind].get(k, low_bit(k))
    bits = [position >> i & 1 for i in range(digits)]
    scalars = {}
    for i in range(digits):
        scalars["bit", i, 0], scalars["bit", i, 1] = bits[i], 1 - bits[i]
    free = {s: [i for i in range(digits) if len({k >> i & 1 for k in raw[s]}) > 1] for s in raw}
    kept = [(c, k) for c in SHARES for k in range(n) if not any(k in raw[s] for s in raw if s[0] == c)]
    for c, k in kept:
        scalars["own", c, k] = (position ^ k) * owned + first[c]
    for s in raw:
        for k in raw[s]:
            to = k ^ by(s[:2], k)
            index = sum((bits[i] ^ (to >> i & 1)) << j for j, i in enumerate(free[s]))
            scalars["got", s, k] = index * rows[s[0]]
    source, scalars = lax.optimization_barrier((grads[0, 0], scalars))
    terms = {key: [] for key in kept}
    held, copied = {}, {}
    sums = lax.optimization_barrier(jnp.zeros((owned, width), jnp.float32))
    state = [x[0] for x in (master, m_codes, v_codes, m_scale, v_scale)]
    weights = jax.ShapeDtypeStruct((n * owned, width), jnp.bfloat16)
    cut = lambda x, at, shape: lax.dynamic_slice(x, at, shape, allow_negative_indices=False)

    def own_piece(c, k):
        return cut(source, (scalars["own", c, k], 0), (rows[c], width))

    def total(c, k):
        own = copied[c, k] if (c, k) in copied else own_piece(c, k)
        return sum((t().astype(jnp.float32) for t in terms[c, k]), own.astype(jnp.float32))

    def block(c, k):
        whole, at = held[c, k]
        return lax.slice_in_dim(whole, at, at + rows[c])

    for step in steps:
        c = step[0]
        if step in raw:
            k, spread = raw[step][0], free[step]
            order = range(digits - 1, -1, -1)
            at = [0 if i in spread else scalars["bit", i, k >> i & 1] for i in order]
            size = [2 if i in spread else 1 for i in order]
            view = source.reshape([2] * digits + [owned, width])
            sent = cut(view, (*at, first[c], 0), (*size, rows[c], width))
            sent = sent.reshape(len(raw[step]) * rows[c], width)
            sent, source = lax.optimization_barrier((sent, source))
        elif step[1] == "s" and step[2:].isdigit():
            k = int(step[2:])
            sent = total(c, k).astype(jnp.bfloat16)
            sent, source = lax.optimization_barrier((sent, source))
        elif step[1] == "o":
            own, source = lax.optimization_barrier((own_piece(c, int(step[2:])), source))
            copied[c, int(step[2:])] = own
        elif step[-1] == "u":
            mine = slice(first[c], first[c] + rows[c])
            summed = total(c, 0)
            w, m, v, ms, vs = (x[mine] for x in state)
            mine = stepped(w, *moments(summed, n, m, ms, v, vs)).astype(jnp.bfloat16)
            sums = lax.dynamic_update_slice(sums, summed, (first[c], 0))
            mine, sums, source, state = lax.optimization_barrier((mine, sums, source, state))
            held[c, 0] = mine, 0
        elif c == "p":
            blocks = [(x[0], int(x[1:])) for x in puts[int(step[1:])]]
            spots = [(k, first[d], rows[d]) for d, k in blocks]
            weights = place(owned, spots, weights, [held[x] for x in blocks])
        elif step in groups:
            blocks = [(x[0], int(x[1:])) for x in groups[step]]
            bit = by(*blocks[0])
            ends = [sum(rows[d] for d, _ in blocks[:i]) for i in range(len(blocks) + 1)]
            sent = jnp.zeros((ends[-1], width), jnp.bfloat16)
            sent = lax.optimization_barrier(sent)
            for (d, k), at in zip(blocks, ends):
                sent = lax.dynamic_update_slice(sent, block(d, k ^ bit), (at, 0))
        elif step == "st":
            w, m, v, ms, vs = state
            one, two = moments(sums, n, m, ms, v, vs)
            master_new = stepped(w, one, two)
            (m_new, m_top), (v_new, v_top) = state_code(one), state_code(two)
        if step in raw:
            got = swap(sent, by(step[:2], k))
            for k in raw[step]:
                terms[c, k ^ by(step[:2], k)].append(
                    lambda got=got, c=c, at=scalars["got", step, k]: cut(
                        got, (at, 0), (rows[c], width)
                    )
                )
        elif step[1] == "s" and step[2:].isdigit():
            bit = by(c + "r", k)
            got = swap(sent, bit)
            terms[c, k ^ bit].append(lambda got=got: got)
        elif step in groups:
            got = swap(sent, bit)
            held.update({key: (got, at) for key, at in zip(blocks, ends)})
        elif sends(step):
            k = int(step[1:])
            bit = by(c, k)
            held[c, k] = swap(block(c, k ^ bit), bit), 0
    return tuple(o[None] for o in (master_new, m_new, m_top, v_new, v_top, weights))


def solution(mesh):
    return jax.shard_map(
        per_device,
        mesh=mesh,
        in_specs=(
            P("dp", "mp", None, None),
            P("mp", "dp", None),
            P("mp", "dp", None),
            P("mp", "dp"),
            P("mp", "dp", None),
            P("mp", "dp"),
        ),
        out_specs=(
            P("mp", "dp", None),
            P("mp", "dp", None),
            P("mp", "dp"),
            P("mp", "dp", None),
            P("mp", "dp"),
            P("mp", None, None),
        ),
        check_vma=False,
    )
```
